32 devices in a mesh: cells: 8 (over z, y), coef: 4 (over x, core).
Axes of the slice: x: 2, y: 2, z: 4, core: 2. Of those that a mesh axis runs over, the one named last changes fastest.
Arguments:
- multipole: bfloat16 [128, 1024], P('coef', 'cells'), may hold values from -6 to 6
- parent_local: bfloat16 [128, 128], P('coef', 'cells'), may hold values from -6 to 6
- m2l_ops: bfloat16 [189, 128, 128], P(None, 'coef'), may hold values from -0.0390625 to 0.0390625
- l2l_ops: bfloat16 [8, 128, 128], P(None, 'coef'), may hold values from -0.5 to 0.5
- target_cell: int32 [189, 1024], P(None, 'cells'), may hold values from -1 to 1023, as said below
- particle_leaf: int32 [16384], P('cells'), may hold values from 0 to 1023, as said below
- particle_basis: bfloat16 [128, 16384], P('coef', 'cells'), may hold values from -0.5 to 0.5
Outputs:
- leaf_local: float32 [128, 1024], P('coef', 'cells')
- potential: float32 [16384], P('cells')
The draws below stay inside these ranges and needn't reach their ends.
Inputs may be any that keep to these rules, and one draw needn't show every extreme that they name: `target_cell`: -1 marks an empty slot. Otherwise the target of source cell c lies on the device of c (cells are owned in blocks of 128: device c // 128) or on a device at most 2 indices away; from one device's source cells at most 256 pairs target the cells of any one other device, and some pair of devices has exactly 256. `particle_leaf`: the particles at positions d * 2048 to (d + 1) * 2048 - 1 lie in cells d * 128 to (d + 1) * 128 - 1.
All inputs are finite; a program needn't handle non-finite values.
Results may differ from the reference program's by a relative error of at most 0.0003.
Values may be sent and summed in bfloat16 or wider, within the bound.
A program may use at most 64 MiB of HBM per device.

```python
import jax
import jax.numpy as jnp
import numpy as np
from jax import lax

K = 128
NOFF = 189
CD = 128
PD = 2048
CAP = 256
REACH = 2
OWNERS = 8
CELLS = 1024
PCELLS = 128
PARTICLES = 16384


def draw_target_cell(key, part):
    moves = jnp.asarray(np.concatenate([np.arange(-REACH, 0), np.arange(1, REACH + 1)]), jnp.int32)
    groups = 2 * REACH
    pairs = NOFF * CD

    def one_device(device):
        device_key = jax.random.fold_in(jax.random.fold_in(key, 11), device)
        keys = jax.random.split(device_key, 5)
        counts = jax.random.randint(keys[0], (groups,), CAP // 4, CAP + 1)
        forced = jax.random.randint(keys[1], (), 0, groups)
        counts = jnp.where(jnp.arange(groups) == forced, CAP, counts)
        dests = device + moves
        inside = (dests >= 0) & (dests < OWNERS)
        counts = jnp.where(inside, counts, 0).astype(jnp.int32)
        ends = jnp.cumsum(counts).astype(jnp.int32)
        order = jax.random.permutation(keys[2], pairs)
        place = jnp.zeros((pairs,), jnp.int32).at[order].set(jnp.arange(pairs, dtype=jnp.int32))
        group = jnp.searchsorted(ends, place, side='right').astype(jnp.int32)
        remote = group < groups
        target_dev = device + moves[jnp.minimum(group, groups - 1)]
        cell = jax.random.randint(keys[3], (pairs,), 0, CD)
        empty = jax.random.randint(keys[4], (pairs,), 0, 8) == 0
        local_target = jnp.where(empty, -1, device * CD + cell)
        result = jnp.where(remote, target_dev * CD + cell, local_target)
        return result.astype(jnp.int32).reshape(NOFF, CD)
    table = lax.map(one_device, jnp.arange(OWNERS, dtype=jnp.int32))
    return jnp.transpose(table, (1, 0, 2)).reshape(NOFF, OWNERS * CD)


def draw_particle_leaf(key, part):
    leaf_key = jax.random.fold_in(key, 23)
    owner = jnp.arange(PD * OWNERS, dtype=jnp.int32) // PD
    cell = jax.random.randint(leaf_key, (PD * OWNERS,), 0, CD)
    return (owner * CD + cell).astype(jnp.int32)


def block_scale(own_key, extent, pieces, smallest, largest):
    gain = 1.0
    for dim, parts in pieces:
        steps = jax.random.uniform(jax.random.fold_in(jax.random.fold_in(own_key, 6), dim), (parts,), jnp.float32, smallest / len(pieces), largest / len(pieces))
        gain = gain * jnp.repeat(jnp.exp(steps), extent[dim] // parts).reshape((-1,) + (1,) * (len(extent) - 1 - dim))
    return gain


def normal_values(stream_key, dims, scale, bound, shards=(), kind=jnp.bfloat16):
    loudness = block_scale(stream_key, dims, shards, -0.22, 0.18) if shards else 1.0
    values = jax.random.normal(stream_key, dims, jnp.float32) * scale * loudness
    return jnp.minimum(jnp.maximum(values, -bound), bound).astype(kind)


def setup_inputs(seed: int = 0) -> dict:
    key_list = jax.random.split(jax.random.key(seed), 8)
    multipole = normal_values(key_list[0], (K, CELLS), 1.0, 6.0, ((0, 4), (1, 8)))
    parent_local = normal_values(key_list[1], (K, PCELLS), 1.0, 6.0, ((0, 4), (1, 8)))
    m2l_ops = normal_values(key_list[2], (NOFF, K, K), (K * NOFF) ** -0.5, 0.0390625, ((1, 4),))
    l2l_ops = normal_values(key_list[3], (8, K, K), K ** -0.5, 0.5, ((1, 4),))
    target_cell = draw_target_cell(jax.random.fold_in(key_list[7], 71), 0)
    particle_leaf = draw_particle_leaf(jax.random.fold_in(key_list[7], 71), 0)
    particle_basis = normal_values(key_list[6], (K, PARTICLES), K ** -0.5, 0.5, ((0, 4), (1, 8)))
    return dict(multipole=multipole, parent_local=parent_local, m2l_ops=m2l_ops, l2l_ops=l2l_ops, target_cell=target_cell, particle_leaf=particle_leaf, particle_basis=particle_basis)


def reference(multipole, parent_local, m2l_ops, l2l_ops, target_cell, particle_leaf, particle_basis):
    width = multipole.shape[0]
    cell_count = multipole.shape[1]
    poles_wide = multipole.astype(jnp.float32)
    parents_wide = parent_local.astype(jnp.float32)

    def offset_step(total, inputs):
        operator, targets = inputs
        term = jnp.dot(operator.astype(jnp.float32), poles_wide, preferred_element_type=jnp.float32)
        index = jnp.where(targets >= 0, targets, cell_count).astype(jnp.int32)
        return total.at[:, index].add(term, mode="drop"), None

    start = jnp.zeros((width, cell_count), jnp.float32)
    m2l_sum, _ = lax.scan(offset_step, start, (m2l_ops, target_cell))
    children = [jnp.dot(l2l_ops[octant].astype(jnp.float32), parents_wide, preferred_element_type=jnp.float32) for octant in range(8)]
    shifted = jnp.stack(children, axis=2).reshape(width, cell_count)
    leaf_local = m2l_sum + shifted
    columns = leaf_local[:, particle_leaf]
    potential = jnp.sum(columns * particle_basis.astype(jnp.float32), axis=0)
    return leaf_local, potential
```

```python
import functools

import jax
import jax.numpy as jnp
from jax import lax
from jax.experimental import pallas as pl
from jax.experimental.pallas import tpu as pltpu
from jax.sharding import PartitionSpec as P

WINDOWS = (-2, 2, -1, 1)
NT = (((1,), (1,)), ((), ()))
TN = (((0,), (0,)), ((), ()))
BF = jnp.bfloat16
HOT = jnp.float8_e4m3fn
MESH = pl.DeviceIdType.MESH


def halves(value):
    high = value.astype(BF)
    low = (value - high.astype(jnp.float32)).astype(BF)
    return high, low


def kernel(
    n_cells, n_coef, group,
    poles_hbm, parents_hbm, ops_hbm, l2l_hbm, target_hbm, leaf_hbm, basis_hbm,
    local_ref, pot_ref,
    ops_ref, l2l_ref, target_ref, leaf_ref, basis_ref,
    gathered, elders, hot_far, hot_near, leaf_hot, outer_ref, rows_ref,
    out_buf, in_buf, partials,
    load_sem, g_send, g_recv, e_send, e_recv, w_send, w_recv, p_send, p_recv,
):
    row = lax.axis_index("cells")
    col = lax.axis_index("coef")
    noff, share, width = ops_ref.shape
    cd = target_ref.shape[1]
    tiles, lanes = leaf_ref.shape

    loads = [
        pltpu.make_async_copy(src, dst, load_sem.at[i])
        for i, (src, dst) in enumerate(
            ((target_hbm, target_ref), (ops_hbm, ops_ref), (l2l_hbm, l2l_ref),
             (leaf_hbm, leaf_ref), (basis_hbm, basis_ref),
             (poles_hbm, gathered.at[col]), (parents_hbm, elders.at[col]))
        )
    ]
    for load in loads:
        load.start()

    barrier = pltpu.get_barrier_semaphore()
    for d in range(1, n_coef):
        pl.semaphore_signal(
            barrier, inc=1, device_id=(row, lax.rem(col + d, n_coef)), device_id_type=MESH
        )
    for w in WINDOWS:
        @pl.when((row + w >= 0) & (row + w < n_cells))
        def _():
            pl.semaphore_signal(barrier, inc=1, device_id=(row + w, col), device_id_type=MESH)
    peers = n_coef - 1
    for w in WINDOWS:
        peers = peers + ((row + w >= 0) & (row + w < n_cells)).astype(jnp.int32)
    pl.semaphore_wait(barrier, peers)

    def gather_copy(k, d, slot):
        src, dst, send, recv = (
            (poles_hbm, gathered, g_send, g_recv), (parents_hbm, elders, e_send, e_recv)
        )[k]
        return pltpu.make_async_remote_copy(
            src_ref=src, dst_ref=dst.at[slot],
            send_sem=send.at[d - 1], recv_sem=recv.at[slot],
            device_id=(row, lax.rem(col + d, n_coef)), device_id_type=MESH,
        )

    for k in range(2):
        for d in range(1, n_coef):
            gather_copy(k, d, col).start()

    def one_hot(line, count):
        wide = jnp.broadcast_to(line, (16, line.shape[1])).astype(BF)
        tall = jnp.concatenate([wide] * (count // 16), axis=0)
        iota = lax.broadcasted_iota(jnp.int32, tall.shape, 0).astype(jnp.float32).astype(BF)
        return jnp.where(tall == iota, jnp.ones_like(tall), jnp.zeros_like(tall)).astype(HOT)

    def span(first):
        return pl.ds(pl.multiple_of(first * cd, cd), cd)

    def fill_far(g):
        first = g * group
        target = target_ref[pl.ds(first, group), :]
        t = target - row * cd
        outer = (t < -cd) | (t >= 2 * cd)
        slot = jnp.where(t < 0, t + jnp.where(outer, 2 * cd, cd), t - jnp.where(outer, cd, 0))
        far = (target >= 0) & ((t < 0) | (t >= cd))
        slot = jnp.where(far, slot, -1).astype(jnp.float32)
        swap = ((t < -cd) | ((t >= cd) & (t < 2 * cd))).astype(jnp.float32)
        for j in range(group):
            hot_far[:, span(first + j)] = one_hot(slot[j : j + 1], 2 * cd)
            outer_ref[:, span(first + j)] = jnp.broadcast_to(
                swap[j : j + 1], (16, cd)
            ).astype(BF)

    def fill_near(g):
        first = g * group
        target = target_ref[pl.ds(first, group), :]
        t = target - row * cd
        slot = jnp.where((target >= 0) & (t >= 0) & (t < cd), t, -1).astype(jnp.float32)
        for j in range(group):
            hot_near[:, span(first + j)] = one_hot(slot[j : j + 1], cd)

    loads[0].wait()
    lax.fori_loop(0, noff // group, lambda g, _: fill_far(g), None)

    loads[5].wait()
    for d in range(1, n_coef):
        gather_copy(0, d, lax.rem(col + d, n_coef)).wait_recv()
    loads[1].wait()

    poles = jnp.concatenate([gathered[j] for j in range(n_coef)], axis=0)
    high, low = halves(
        jnp.dot(ops_ref[...].reshape(noff * share, width), poles,
                preferred_element_type=jnp.float32)
    )
    for j in range(noff):
        both = jnp.concatenate(
            [part[j * share : (j + 1) * share] for part in (high, low)], axis=0
        )
        rows_ref[: 2 * share, j * cd : (j + 1) * cd] = both
        keep = jnp.concatenate([outer_ref[:, j * cd : (j + 1) * cd]] * (2 * share // 16), axis=0)
        rows_ref[2 * share :, j * cd : (j + 1) * cd] = both * keep

    def window_copy(i, w):
        return pltpu.make_async_remote_copy(
            src_ref=out_buf.at[i], dst_ref=in_buf.at[i],
            send_sem=w_send.at[i], recv_sem=w_recv.at[i],
            device_id=(row + w, col), device_id_type=MESH,
        )

    sums = lax.dot_general(rows_ref[...], hot_far[...], NT, preferred_element_type=jnp.float32)
    every = sums[:share] + sums[share : 2 * share]
    some = sums[2 * share : 3 * share] + sums[3 * share :]
    rest = every - some
    for i, part in enumerate((some[:, :cd], rest[:, cd:], rest[:, :cd], some[:, cd:])):
        out_buf[i] = part
    for i, w in enumerate(WINDOWS):
        @pl.when((row + w >= 0) & (row + w < n_cells))
        def _():
            window_copy(i, w).start()

    lax.fori_loop(0, noff // group, lambda g, _: fill_near(g), None)
    sums = lax.dot_general(
        rows_ref[: 2 * share, :], hot_near[...], NT, preferred_element_type=jnp.float32
    )
    total = sums[:share] + sums[share:]

    loads[2].wait()
    loads[6].wait()
    for d in range(1, n_coef):
        gather_copy(1, d, lax.rem(col + d, n_coef)).wait_recv()
    held = (elders.shape[1], cd)
    child = lax.broadcasted_iota(jnp.int32, held, 1)
    family = child // 8 == lax.broadcasted_iota(jnp.int32, held, 0)
    family = family.astype(jnp.float32).astype(BF)
    wide_parents = jnp.concatenate(
        [
            lax.dot_general(elders[j], family, TN, preferred_element_type=jnp.float32)
            for j in range(n_coef)
        ],
        axis=0,
    )
    octant = lax.broadcasted_iota(jnp.int32, wide_parents.shape, 1) % 8
    spread = jnp.concatenate(
        [jnp.where(octant == j, wide_parents, 0.0).astype(BF) for j in range(8)], axis=0
    )
    shifts = jnp.concatenate([l2l_ref[j] for j in range(8)], axis=1)
    total = total + jnp.dot(shifts, spread, preferred_element_type=jnp.float32)
    local_ref[...] = total

    loads[3].wait()
    for t in range(tiles):
        leaf = (leaf_ref[t : t + 1, :] - row * cd).astype(jnp.float32)
        leaf_hot[:, t * lanes : (t + 1) * lanes] = one_hot(leaf, cd)
    loads[4].wait()

    for i, w in enumerate(WINDOWS):
        @pl.when((row - w >= 0) & (row - w < n_cells))
        def _():
            window_copy(i, w).wait_recv()
            local_ref[...] += in_buf[i]

    columns = jnp.dot(
        jnp.concatenate(halves(local_ref[...]), axis=0), leaf_hot[...],
        preferred_element_type=jnp.float32,
    )
    columns = columns[:share] + columns[share:]
    partial = jnp.sum(columns * basis_ref[...].astype(jnp.float32), axis=0, keepdims=True)
    partials[col] = jnp.concatenate(
        [partial[:, t * lanes : (t + 1) * lanes] for t in range(tiles)], axis=0
    )

    def partial_copy(d, slot):
        return pltpu.make_async_remote_copy(
            src_ref=partials.at[slot], dst_ref=partials.at[slot],
            send_sem=p_send.at[d - 1], recv_sem=p_recv.at[slot],
            device_id=(row, lax.rem(col + d, n_coef)), device_id_type=MESH,
        )

    for d in range(1, n_coef):
        partial_copy(d, col).start()
    for d in range(1, n_coef):
        partial_copy(d, lax.rem(col + d, n_coef)).wait_recv()
    potential = partials[0]
    for j in range(1, n_coef):
        potential = potential + partials[j]
    pot_ref[...] = potential

    for d in range(1, n_coef):
        gather_copy(0, d, col).wait_send()
        gather_copy(1, d, col).wait_send()
        partial_copy(d, col).wait_send()
    for i, w in enumerate(WINDOWS):
        @pl.when((row + w >= 0) & (row + w < n_cells))
        def _():
            window_copy(i, w).wait_send()


def on_device(
    n_cells, n_coef,
    multipole, parent_local, m2l_ops, l2l_ops, target_cell, particle_leaf, particle_basis,
):
    share, cd = multipole.shape
    noff = m2l_ops.shape[0]
    particles = particle_leaf.shape[0]
    lanes = 128
    tiles = particles // lanes
    group = max(g for g in range(1, 33) if noff % g == 0)
    leaf = particle_leaf.reshape(tiles, lanes)
    nwin = len(WINDOWS)
    dma = pltpu.SemaphoreType.DMA
    vmem = pl.BlockSpec(memory_space=pltpu.VMEM)
    hbm = pl.BlockSpec(memory_space=pltpu.HBM)
    local, potential = pl.pallas_call(
        functools.partial(kernel, n_cells, n_coef, group),
        out_shape=(pltpu.VMEM((share, cd), jnp.float32), pltpu.VMEM((tiles, lanes), jnp.float32)),
        in_specs=[hbm] * 7,
        out_specs=(vmem, vmem),
        scratch_shapes=[
            pltpu.VMEM(m2l_ops.shape, m2l_ops.dtype),
            pltpu.VMEM(l2l_ops.shape, l2l_ops.dtype),
            pltpu.VMEM(target_cell.shape, target_cell.dtype),
            pltpu.VMEM(leaf.shape, leaf.dtype),
            pltpu.VMEM(particle_basis.shape, particle_basis.dtype),
            pltpu.VMEM((n_coef, share, cd), BF),
            pltpu.VMEM((n_coef,) + parent_local.shape[::-1], BF),
            pltpu.VMEM((2 * cd, noff * cd), HOT),
            pltpu.VMEM((cd, noff * cd), HOT),
            pltpu.VMEM((cd, particles), HOT),
            pltpu.VMEM((16, noff * cd), BF),
            pltpu.VMEM((4 * share, noff * cd), BF),
            pltpu.VMEM((nwin, share, cd), jnp.float32),
            pltpu.VMEM((nwin, share, cd), jnp.float32),
            pltpu.VMEM((n_coef, tiles, lanes), jnp.float32),
            dma((7,)),
            dma((n_coef - 1,)),
            dma((n_coef,)),
            dma((n_coef - 1,)),
            dma((n_coef,)),
            dma((nwin,)),
            dma((nwin,)),
            dma((n_coef - 1,)),
            dma((n_coef,)),
        ],
        compiler_params=pltpu.CompilerParams(
            collective_id=0, has_side_effects=True, vmem_limit_bytes=60000000
        ),
    )(multipole, parent_local.T, m2l_ops, l2l_ops, target_cell, leaf, particle_basis)
    return local, potential.reshape(particles)


def solution(mesh):
    return jax.shard_map(
        functools.partial(on_device, mesh.shape["cells"], mesh.shape["coef"]),
        mesh=mesh,
        in_specs=(
            P("coef", "cells"),
            P("coef", "cells"),
            P(None, "coef", None),
            P(None, "coef", None),
            P(None, "cells"),
            P("cells"),
            P("coef", "cells"),
        ),
        out_specs=(P("coef", "cells"), P("cells")),
        check_vma=False,
    )
```

```python
import functools

import jax
import jax.numpy as jnp
from jax import lax
from jax.experimental import pallas as pl
from jax.experimental.pallas import tpu as pltpu
from jax.sharding import PartitionSpec as P

WINDOWS = (-1, 1, -2, 2)
NT = (((1,), (1,)), ((), ()))
TN = (((0,), (0,)), ((), ()))
BF = jnp.bfloat16
HOT = jnp.float8_e4m3fn
MESH = pl.DeviceIdType.MESH


def halves(value):
    high = value.astype(BF)
    low = (value - high.astype(jnp.float32)).astype(BF)
    return high, low


def kernel(
    n_cells, n_coef, group,
    poles_hbm, parents_hbm, ops_hbm, l2l_hbm, target_hbm, leaf_hbm, basis_hbm,
    local_ref, pot_ref,
    ops_ref, l2l_ref, target_ref, leaf_ref, basis_ref,
    gathered, elders, hot_far, hot_near, leaf_hot, outer_ref, rows_ref,
    out_buf, in_buf, partials,
    load_sem, g_send, g_recv, e_send, e_recv, w_send, w_recv, p_send, p_recv,
):
    row = lax.axis_index("cells")
    col = lax.axis_index("coef")
    noff, share, width = ops_ref.shape
    cd = target_ref.shape[1]
    tiles, lanes = leaf_ref.shape

    loads = [
        pltpu.make_async_copy(src, dst, load_sem.at[i])
        for i, (src, dst) in enumerate(
            ((poles_hbm, gathered.at[col]), (parents_hbm, elders.at[col]),
             (target_hbm, target_ref), (leaf_hbm, leaf_ref), (ops_hbm, ops_ref),
             (l2l_hbm, l2l_ref), (basis_hbm, basis_ref))
        )
    ]
    for load in loads:
        load.start()

    barrier = pltpu.get_barrier_semaphore()
    for d in range(1, n_coef):
        pl.semaphore_signal(
            barrier, inc=1, device_id=(row, lax.rem(col + d, n_coef)), device_id_type=MESH
        )
    for w in WINDOWS:
        @pl.when((row + w >= 0) & (row + w < n_cells))
        def _():
            pl.semaphore_signal(barrier, inc=1, device_id=(row + w, col), device_id_type=MESH)
    peers = n_coef - 1
    for w in WINDOWS:
        peers = peers + ((row + w >= 0) & (row + w < n_cells)).astype(jnp.int32)
    pl.semaphore_wait(barrier, peers)
    loads[0].wait()
    loads[1].wait()

    def gather_copy(k, d, slot):
        src, dst, send, recv = (
            (gathered.at[col], gathered, g_send, g_recv),
            (elders.at[col], elders, e_send, e_recv),
        )[k]
        return pltpu.make_async_remote_copy(
            src_ref=src, dst_ref=dst.at[slot],
            send_sem=send.at[d - 1], recv_sem=recv.at[slot],
            device_id=(row, lax.rem(col + d, n_coef)), device_id_type=MESH,
        )

    for k in range(2):
        for d in range(1, n_coef):
            gather_copy(k, d, col).start()

    def one_hot(line, count, value=1.0):
        wide = jnp.broadcast_to(line, (16, line.shape[1])).astype(BF)
        tall = jnp.concatenate([wide] * (count // 16), axis=0)
        iota = lax.broadcasted_iota(jnp.int32, tall.shape, 0).astype(jnp.float32).astype(BF)
        hit = jnp.full(tall.shape, value, jnp.float32).astype(BF)
        return jnp.where(tall == iota, hit, jnp.zeros_like(tall)).astype(HOT)

    half = 2 * pl.cdiv(noff, 4)

    def sign(j):
        return jnp.where(j < half, 1.0, -1.0)


    def fill_far(g):
        first = g * group
        target = target_ref[pl.ds(first, group), :]
        t = target - row * cd
        outer = (t < -cd) | (t >= 2 * cd)
        slot = jnp.where(t < 0, t + jnp.where(outer, 2 * cd, cd), t - jnp.where(outer, cd, 0))
        far = (target >= 0) & ((t < 0) | (t >= cd))
        slot = jnp.where(far, slot, -1).astype(jnp.float32)
        swap = ((t < -cd) | ((t >= cd) & (t < 2 * cd))).astype(jnp.float32)
        for j in range(group):
            hot_far[first + j] = one_hot(
                slot[j : j + 1], 2 * cd, sign(first + j)
            )
            outer_ref[first + j] = jnp.broadcast_to(
                swap[j : j + 1], (16, cd)
            ).astype(BF)

    def fill_near(g):
        first = g * group
        target = target_ref[pl.ds(first, group), :]
        t = target - row * cd
        slot = jnp.where((target >= 0) & (t >= 0) & (t < cd), t, -1).astype(jnp.float32)
        for j in range(group):
            hot_near[first + j] = one_hot(slot[j : j + 1], cd, sign(first + j))

    loads[2].wait()
    lax.fori_loop(0, noff // group, lambda g, _: fill_far(g), None)
    lax.fori_loop(0, noff // group, lambda g, _: fill_near(g), None)
    loads[3].wait()
    for t in range(tiles):
        leaf = (leaf_ref[t : t + 1, :] - row * cd).astype(jnp.float32)
        leaf_hot[:, t * lanes : (t + 1) * lanes] = one_hot(leaf, cd)

    for d in range(1, n_coef):
        gather_copy(0, d, lax.rem(col + d, n_coef)).wait_recv()
    loads[4].wait()

    poles = jnp.concatenate([gathered[j] for j in range(n_coef)], axis=0)
    high, low = halves(
        jnp.dot(ops_ref[...].reshape(noff * share, width), poles,
                preferred_element_type=jnp.float32)
    )
    for j in range(noff):
        both = jnp.concatenate(
            [part[j * share : (j + 1) * share] for part in (high, low)], axis=0
        )
        keep = jnp.concatenate([outer_ref[j]] * (2 * share // 16), axis=0)
        rows_ref[j] = jnp.concatenate([both, both * keep], axis=0)

    def window_copy(i, w):
        return pltpu.make_async_remote_copy(
            src_ref=out_buf.at[i], dst_ref=in_buf.at[i],
            send_sem=w_send.at[i], recv_sem=w_recv.at[i],
            device_id=(row + w, col), device_id_type=MESH,
        )

    def beside(ref, count, first, last):
        return jnp.concatenate([ref[j, :count] for j in range(first, last)], axis=1)

    def scatter(hot, count):
        plus, minus = (
            lax.dot_general(
                beside(rows_ref, count, *part), beside(hot, hot.shape[1], *part), NT,
                preferred_element_type=jnp.float32,
            )
            for part in ((0, half), (half, noff))
        )
        return plus - minus

    sums = scatter(hot_far, 4 * share)
    every = sums[:share] + sums[share : 2 * share]
    some = sums[2 * share : 3 * share] + sums[3 * share :]
    rest = every - some
    for i, part in enumerate((rest[:, :cd], some[:, cd:], some[:, :cd], rest[:, cd:])):
        out_buf[i] = part
    for i, w in enumerate(WINDOWS):
        @pl.when((row + w >= 0) & (row + w < n_cells))
        def _():
            window_copy(i, w).start()

    loads[5].wait()
    loads[6].wait()
    for d in range(1, n_coef):
        gather_copy(1, d, lax.rem(col + d, n_coef)).wait_recv()
    sums = scatter(hot_near, 2 * share)
    total = sums[:share] + sums[share:]

    held = (elders.shape[1], cd)
    child = lax.broadcasted_iota(jnp.int32, held, 1)
    family = child // 8 == lax.broadcasted_iota(jnp.int32, held, 0)
    family = family.astype(jnp.float32).astype(BF)
    wide_parents = jnp.concatenate(
        [
            lax.dot_general(elders[j], family, TN, preferred_element_type=jnp.float32)
            for j in range(n_coef)
        ],
        axis=0,
    )
    octant = lax.broadcasted_iota(jnp.int32, wide_parents.shape, 1) % 8
    spread = jnp.concatenate(
        [jnp.where(octant == j, wide_parents, 0.0).astype(BF) for j in range(8)], axis=0
    )
    shifts = jnp.concatenate([l2l_ref[j] for j in range(8)], axis=1)
    total = total + jnp.dot(shifts, spread, preferred_element_type=jnp.float32)
    local_ref[...] = total

    for i, w in enumerate(WINDOWS):
        @pl.when((row - w >= 0) & (row - w < n_cells))
        def _():
            window_copy(i, w).wait_recv()
            local_ref[...] += in_buf[i]

    columns = jnp.dot(
        jnp.concatenate(halves(local_ref[...]), axis=0), leaf_hot[...],
        preferred_element_type=jnp.float32,
    )
    columns = columns[:share] + columns[share:]
    partial = jnp.sum(columns * basis_ref[...].astype(jnp.float32), axis=0, keepdims=True)
    partials[col] = jnp.concatenate(
        [partial[:, t * lanes : (t + 1) * lanes] for t in range(tiles)], axis=0
    )

    def partial_copy(d, slot):
        return pltpu.make_async_remote_copy(
            src_ref=partials.at[slot], dst_ref=partials.at[slot],
            send_sem=p_send.at[d - 1], recv_sem=p_recv.at[slot],
            device_id=(row, lax.rem(col + d, n_coef)), device_id_type=MESH,
        )

    for d in range(1, n_coef):
        partial_copy(d, col).start()
    for d in range(1, n_coef):
        partial_copy(d, lax.rem(col + d, n_coef)).wait_recv()
    potential = partials[0]
    for j in range(1, n_coef):
        potential = potential + partials[j]
    pot_ref[...] = potential

    for d in range(1, n_coef):
        gather_copy(0, d, col).wait_send()
        gather_copy(1, d, col).wait_send()
        partial_copy(d, col).wait_send()
    for i, w in enumerate(WINDOWS):
        @pl.when((row + w >= 0) & (row + w < n_cells))
        def _():
            window_copy(i, w).wait_send()


def on_device(
    n_cells, n_coef,
    multipole, parent_local, m2l_ops, l2l_ops, target_cell, particle_leaf, particle_basis,
):
    share, cd = multipole.shape
    noff = m2l_ops.shape[0]
    particles = particle_leaf.shape[0]
    lanes = 128
    tiles = particles // lanes
    group = max(g for g in range(1, 33) if noff % g == 0)
    leaf = particle_leaf.reshape(tiles, lanes)
    nwin = len(WINDOWS)
    dma = pltpu.SemaphoreType.DMA
    vmem = pl.BlockSpec(memory_space=pltpu.VMEM)
    hbm = pl.BlockSpec(memory_space=pltpu.HBM)
    local, potential = pl.pallas_call(
        functools.partial(kernel, n_cells, n_coef, group),
        out_shape=(pltpu.VMEM((share, cd), jnp.float32), pltpu.VMEM((tiles, lanes), jnp.float32)),
        in_specs=[hbm] * 7,
        out_specs=(vmem, vmem),
        scratch_shapes=[
            pltpu.VMEM(m2l_ops.shape, m2l_ops.dtype),
            pltpu.VMEM(l2l_ops.shape, l2l_ops.dtype),
            pltpu.VMEM(target_cell.shape, target_cell.dtype),
            pltpu.VMEM(leaf.shape, leaf.dtype),
            pltpu.VMEM(particle_basis.shape, particle_basis.dtype),
            pltpu.VMEM((n_coef, share, cd), BF),
            pltpu.VMEM((n_coef,) + parent_local.shape[::-1], BF),
            pltpu.VMEM((noff, 2 * cd, cd), HOT),
            pltpu.VMEM((noff, cd, cd), HOT),
            pltpu.VMEM((cd, particles), HOT),
            pltpu.VMEM((noff, 16, cd), BF),
            pltpu.VMEM((noff, 4 * share, cd), BF),
            pltpu.VMEM((nwin, share, cd), jnp.float32),
            pltpu.VMEM((nwin, share, cd), jnp.float32),
            pltpu.VMEM((n_coef, tiles, lanes), jnp.float32),
            dma((7,)),
            dma((n_coef - 1,)),
            dma((n_coef,)),
            dma((n_coef - 1,)),
            dma((n_coef,)),
            dma((nwin,)),
            dma((nwin,)),
            dma((n_coef - 1,)),
            dma((n_coef,)),
        ],
        compiler_params=pltpu.CompilerParams(
            collective_id=0, has_side_effects=True, vmem_limit_bytes=60000000
        ),
    )(multipole, parent_local.T, m2l_ops, l2l_ops, target_cell, leaf, particle_basis)
    return local, potential.reshape(particles)


def solution(mesh):
    return jax.shard_map(
        functools.partial(on_device, mesh.shape["cells"], mesh.shape["coef"]),
        mesh=mesh,
        in_specs=(
            P("coef", "cells"),
            P("coef", "cells"),
            P(None, "coef", None),
            P(None, "coef", None),
            P(None, "cells"),
            P("cells"),
            P("coef", "cells"),
        ),
        out_specs=(P("coef", "cells"), P("cells")),
        check_vma=False,
    )
```

```python
import functools

import jax
import jax.numpy as jnp
from jax import lax
from jax.experimental import pallas as pl
from jax.experimental.pallas import tpu as pltpu
from jax.sharding import PartitionSpec as P

WINDOWS = (-2, 2, -1, 1)
NT = (((1,), (1,)), ((), ()))
TN = (((0,), (0,)), ((), ()))
BF = jnp.bfloat16
HOT = jnp.float8_e4m3fn
MESH = pl.DeviceIdType.MESH


def halves(value):
    high = value.astype(BF)
    low = (value - high.astype(jnp.float32)).astype(BF)
    return high, low


def kernel(
    n_cells, n_coef, group,
    poles_hbm, parents_hbm, ops_hbm, l2l_hbm, target_hbm, leaf_hbm, basis_hbm,
    local_ref, pot_ref,
    ops_ref, l2l_ref, target_ref, leaf_ref, basis_ref,
    gathered, elders, hot_far, hot_near, leaf_hot, outer_ref, rows_ref,
    out_buf, in_buf, partials,
    load_sem, g_send, g_recv, e_send, e_recv, w_send, w_recv, p_send, p_recv,
):
    row = lax.axis_index("cells")
    col = lax.axis_index("coef")
    noff, share, width = ops_ref.shape
    cd = target_ref.shape[1]
    tiles, lanes = leaf_ref.shape

    loads = [
        pltpu.make_async_copy(src, dst, load_sem.at[i])
        for i, (src, dst) in enumerate(
            ((poles_hbm, gathered.at[col]), (parents_hbm, elders.at[col]),
             (target_hbm, target_ref), (leaf_hbm, leaf_ref), (ops_hbm, ops_ref),
             (l2l_hbm, l2l_ref), (basis_hbm, basis_ref))
        )
    ]
    for load in loads:
        load.start()

    barrier = pltpu.get_barrier_semaphore()
    for d in range(1, n_coef):
        pl.semaphore_signal(
            barrier, inc=1, device_id=(row, lax.rem(col + d, n_coef)), device_id_type=MESH
        )
    for w in WINDOWS:
        @pl.when((row + w >= 0) & (row + w < n_cells))
        def _():
            pl.semaphore_signal(barrier, inc=1, device_id=(row + w, col), device_id_type=MESH)
    peers = n_coef - 1
    for w in WINDOWS:
        peers = peers + ((row + w >= 0) & (row + w < n_cells)).astype(jnp.int32)
    pl.semaphore_wait(barrier, peers)
    loads[0].wait()
    loads[1].wait()

    def gather_copy(k, d, slot):
        src, dst, send, recv = (
            (gathered.at[col], gathered, g_send, g_recv),
            (elders.at[col], elders, e_send, e_recv),
        )[k]
        return pltpu.make_async_remote_copy(
            src_ref=src, dst_ref=dst.at[slot],
            send_sem=send.at[d - 1], recv_sem=recv.at[slot],
            device_id=(row, lax.rem(col + d, n_coef)), device_id_type=MESH,
        )

    for k in range(2):
        for d in range(1, n_coef):
            gather_copy(k, d, col).start()

    def one_hot(line, count, value=1.0):
        wide = jnp.broadcast_to(line, (16, line.shape[1])).astype(BF)
        tall = jnp.concatenate([wide] * (count // 16), axis=0)
        iota = lax.broadcasted_iota(jnp.int32, tall.shape, 0).astype(jnp.float32).astype(BF)
        hit = jnp.full(tall.shape, value, jnp.float32).astype(BF)
        return jnp.where(tall == iota, hit, jnp.zeros_like(tall)).astype(HOT)

    half = 2 * pl.cdiv(noff, 4)

    def sign(j):
        return jnp.where(j < half, 1.0, -1.0)


    def fill_far(g):
        first = g * group
        target = target_ref[pl.ds(first, group), :]
        t = target - row * cd
        outer = (t < -cd) | (t >= 2 * cd)
        slot = jnp.where(t < 0, t + jnp.where(outer, 2 * cd, cd), t - jnp.where(outer, cd, 0))
        far = (target >= 0) & ((t < 0) | (t >= cd))
        slot = jnp.where(far, slot, -1).astype(jnp.float32)
        swap = ((t < -cd) | ((t >= cd) & (t < 2 * cd))).astype(jnp.float32)
        for j in range(group):
            hot_far[first + j] = one_hot(
                slot[j : j + 1], 2 * cd, sign(first + j)
            )
            outer_ref[first + j] = jnp.broadcast_to(
                swap[j : j + 1], (16, cd)
            ).astype(BF)

    def fill_near(g):
        first = g * group
        target = target_ref[pl.ds(first, group), :]
        t = target - row * cd
        slot = jnp.where((target >= 0) & (t >= 0) & (t < cd), t, -1).astype(jnp.float32)
        for j in range(group):
            hot_near[first + j] = one_hot(slot[j : j + 1], cd, sign(first + j))

    loads[2].wait()
    lax.fori_loop(0, noff // group, lambda g, _: fill_far(g), None)
    lax.fori_loop(0, noff // group, lambda g, _: fill_near(g), None)
    loads[3].wait()
    for t in range(tiles):
        leaf = (leaf_ref[t : t + 1, :] - row * cd).astype(jnp.float32)
        leaf_hot[:, t * lanes : (t + 1) * lanes] = one_hot(leaf, cd)

    for d in range(1, n_coef):
        gather_copy(0, d, lax.rem(col + d, n_coef)).wait_recv()
    loads[4].wait()

    poles = jnp.concatenate([gathered[j] for j in range(n_coef)], axis=0)
    high, low = halves(
        jnp.dot(ops_ref[...].reshape(noff * share, width), poles,
                preferred_element_type=jnp.float32)
    )
    for j in range(noff):
        both = jnp.concatenate(
            [part[j * share : (j + 1) * share] for part in (high, low)], axis=0
        )
        keep = jnp.concatenate([outer_ref[j]] * (2 * share // 16), axis=0)
        rows_ref[j] = jnp.concatenate([both, both * keep], axis=0)

    def window_copy(i, w):
        return pltpu.make_async_remote_copy(
            src_ref=out_buf.at[i], dst_ref=in_buf.at[i],
            send_sem=w_send.at[i], recv_sem=w_recv.at[i],
            device_id=(row + w, col), device_id_type=MESH,
        )

    def beside(ref, count, first, last):
        return jnp.concatenate([ref[j, :count] for j in range(first, last)], axis=1)

    def scatter(hot, count):
        plus, minus = (
            lax.dot_general(
                beside(rows_ref, count, *part), beside(hot, hot.shape[1], *part), NT,
                preferred_element_type=jnp.float32,
            )
            for part in ((0, half), (half, noff))
        )
        return plus - minus

    sums = scatter(hot_far, 4 * share)
    every = sums[:share] + sums[share : 2 * share]
    some = sums[2 * share : 3 * share] + sums[3 * share :]
    rest = every - some
    for i, part in enumerate((some[:, :cd], rest[:, cd:], rest[:, :cd], some[:, cd:])):
        out_buf[i] = part
    for i, w in enumerate(WINDOWS):
        @pl.when((row + w >= 0) & (row + w < n_cells))
        def _():
            window_copy(i, w).start()

    loads[5].wait()
    loads[6].wait()
    for d in range(1, n_coef):
        gather_copy(1, d, lax.rem(col + d, n_coef)).wait_recv()
    sums = scatter(hot_near, 2 * share)
    total = sums[:share] + sums[share:]

    held = (elders.shape[1], cd)
    child = lax.broadcasted_iota(jnp.int32, held, 1)
    family = child // 8 == lax.broadcasted_iota(jnp.int32, held, 0)
    family = family.astype(jnp.float32).astype(BF)
    wide_parents = jnp.concatenate(
        [
            lax.dot_general(elders[j], family, TN, preferred_element_type=jnp.float32)
            for j in range(n_coef)
        ],
        axis=0,
    )
    octant = lax.broadcasted_iota(jnp.int32, wide_parents.shape, 1) % 8
    spread = jnp.concatenate(
        [jnp.where(octant == j, wide_parents, 0.0).astype(BF) for j in range(8)], axis=0
    )
    shifts = jnp.concatenate([l2l_ref[j] for j in range(8)], axis=1)
    total = total + jnp.dot(shifts, spread, preferred_element_type=jnp.float32)
    local_ref[...] = total

    for i, w in enumerate(WINDOWS):
        @pl.when((row - w >= 0) & (row - w < n_cells))
        def _():
            window_copy(i, w).wait_recv()
            local_ref[...] += in_buf[i]

    columns = jnp.dot(
        jnp.concatenate(halves(local_ref[...]), axis=0), leaf_hot[...],
        preferred_element_type=jnp.float32,
    )
    columns = columns[:share] + columns[share:]
    partial = jnp.sum(columns * basis_ref[...].astype(jnp.float32), axis=0, keepdims=True)
    partials[col] = jnp.concatenate(
        [partial[:, t * lanes : (t + 1) * lanes] for t in range(tiles)], axis=0
    )

    def partial_copy(d, slot):
        return pltpu.make_async_remote_copy(
            src_ref=partials.at[slot], dst_ref=partials.at[slot],
            send_sem=p_send.at[d - 1], recv_sem=p_recv.at[slot],
            device_id=(row, lax.rem(col + d, n_coef)), device_id_type=MESH,
        )

    for d in range(1, n_coef):
        partial_copy(d, col).start()
    for d in range(1, n_coef):
        partial_copy(d, lax.rem(col + d, n_coef)).wait_recv()
    potential = partials[0]
    for j in range(1, n_coef):
        potential = potential + partials[j]
    pot_ref[...] = potential

    for d in range(1, n_coef):
        gather_copy(0, d, col).wait_send()
        gather_copy(1, d, col).wait_send()
        partial_copy(d, col).wait_send()
    for i, w in enumerate(WINDOWS):
        @pl.when((row + w >= 0) & (row + w < n_cells))
        def _():
            window_copy(i, w).wait_send()


def on_device(
    n_cells, n_coef,
    multipole, parent_local, m2l_ops, l2l_ops, target_cell, particle_leaf, particle_basis,
):
    share, cd = multipole.shape
    noff = m2l_ops.shape[0]
    particles = particle_leaf.shape[0]
    lanes = 128
    tiles = particles // lanes
    group = max(g for g in range(1, 33) if noff % g == 0)
    leaf = particle_leaf.reshape(tiles, lanes)
    nwin = len(WINDOWS)
    dma = pltpu.SemaphoreType.DMA
    vmem = pl.BlockSpec(memory_space=pltpu.VMEM)
    hbm = pl.BlockSpec(memory_space=pltpu.HBM)
    local, potential = pl.pallas_call(
        functools.partial(kernel, n_cells, n_coef, group),
        out_shape=(pltpu.VMEM((share, cd), jnp.float32), pltpu.VMEM((tiles, lanes), jnp.float32)),
        in_specs=[hbm] * 7,
        out_specs=(vmem, vmem),
        scratch_shapes=[
            pltpu.VMEM(m2l_ops.shape, m2l_ops.dtype),
            pltpu.VMEM(l2l_ops.shape, l2l_ops.dtype),
            pltpu.VMEM(target_cell.shape, target_cell.dtype),
            pltpu.VMEM(leaf.shape, leaf.dtype),
            pltpu.VMEM(particle_basis.shape, particle_basis.dtype),
            pltpu.VMEM((n_coef, share, cd), BF),
            pltpu.VMEM((n_coef,) + parent_local.shape[::-1], BF),
            pltpu.VMEM((noff, 2 * cd, cd), HOT),
            pltpu.VMEM((noff, cd, cd), HOT),
            pltpu.VMEM((cd, particles), HOT),
            pltpu.VMEM((noff, 16, cd), BF),
            pltpu.VMEM((noff, 4 * share, cd), BF),
            pltpu.VMEM((nwin, share, cd), jnp.float32),
            pltpu.VMEM((nwin, share, cd), jnp.float32),
            pltpu.VMEM((n_coef, tiles, lanes), jnp.float32),
            dma((7,)),
            dma((n_coef - 1,)),
            dma((n_coef,)),
            dma((n_coef - 1,)),
            dma((n_coef,)),
            dma((nwin,)),
            dma((nwin,)),
            dma((n_coef - 1,)),
            dma((n_coef,)),
        ],
        compiler_params=pltpu.CompilerParams(
            collective_id=0, has_side_effects=True, vmem_limit_bytes=60000000
        ),
    )(multipole, parent_local.T, m2l_ops, l2l_ops, target_cell, leaf, particle_basis)
    def put(a, b, c, d, sem):
        one = pltpu.make_async_copy(a, c, sem.at[0])
        two = pltpu.make_async_copy(b, d, sem.at[1])
        one.start()
        two.start()
        one.wait()
        two.wait()

    local = pltpu.with_memory_space_constraint(local, pltpu.VMEM)
    potential = pltpu.with_memory_space_constraint(potential, pltpu.VMEM)
    local, potential = pl.pallas_call(
        put,
        out_shape=(
            jax.ShapeDtypeStruct(local.shape, local.dtype),
            jax.ShapeDtypeStruct(potential.shape, potential.dtype),
        ),
        in_specs=[vmem, vmem],
        out_specs=(hbm, hbm),
        scratch_shapes=[dma((2,))],
    )(local, potential)
    return local, potential.reshape(particles)


def solution(mesh):
    return jax.shard_map(
        functools.partial(on_device, mesh.shape["cells"], mesh.shape["coef"]),
        mesh=mesh,
        in_specs=(
            P("coef", "cells"),
            P("coef", "cells"),
            P(None, "coef", None),
            P(None, "coef", None),
            P(None, "cells"),
            P("cells"),
            P("coef", "cells"),
        ),
        out_specs=(P("coef", "cells"), P("cells")),
        check_vma=False,
    )
```

```python
import functools

import jax
import jax.numpy as jnp
from jax import lax
from jax.experimental import pallas as pl
from jax.experimental.pallas import tpu as pltpu
from jax.sharding import PartitionSpec as P

WINDOWS = (-2, 2, -1, 1)
NT = (((1,), (1,)), ((), ()))
TN = (((0,), (0,)), ((), ()))
BF = jnp.bfloat16
HOT = jnp.float8_e4m3fn
MESH = pl.DeviceIdType.MESH


def halves(value):
    high = value.astype(BF)
    low = (value - high.astype(jnp.float32)).astype(BF)
    return high, low


def kernel(
    n_cells, n_coef, group,
    poles_hbm, parents_hbm, ops_hbm, l2l_hbm, target_hbm, leaf_hbm, basis_hbm,
    local_ref, pot_ref,
    ops_ref, l2l_ref, target_ref, leaf_ref, basis_ref,
    gathered, elders, hot_far, hot_near, leaf_hot, outer_ref, rows_ref,
    out_buf, in_buf, partials,
    load_sem, g_send, g_recv, e_send, e_recv, w_send, w_recv, p_send, p_recv,
):
    row = lax.axis_index("cells")
    col = lax.axis_index("coef")
    noff, share, width = ops_ref.shape
    cd = target_ref.shape[1]
    tiles, lanes = leaf_ref.shape

    barrier = pltpu.get_barrier_semaphore()
    for d in range(1, n_coef):
        pl.semaphore_signal(
            barrier, inc=1, device_id=(row, lax.rem(col + d, n_coef)), device_id_type=MESH
        )
    for w in WINDOWS:
        @pl.when((row + w >= 0) & (row + w < n_cells))
        def _():
            pl.semaphore_signal(barrier, inc=1, device_id=(row + w, col), device_id_type=MESH)
    loads = [
        pltpu.make_async_copy(src, dst, load_sem.at[i])
        for i, (src, dst) in enumerate(
            ((poles_hbm, gathered.at[col]), (parents_hbm, elders.at[col]),
             (target_hbm, target_ref), (leaf_hbm, leaf_ref), (ops_hbm, ops_ref),
             (l2l_hbm, l2l_ref), (basis_hbm, basis_ref))
        )
    ]
    for load in loads:
        load.start()

    peers = n_coef - 1
    for w in WINDOWS:
        peers = peers + ((row + w >= 0) & (row + w < n_cells)).astype(jnp.int32)
    pl.semaphore_wait(barrier, peers)
    loads[0].wait()
    loads[1].wait()

    def gather_copy(k, d, slot):
        src, dst, send, recv = (
            (gathered.at[col], gathered, g_send, g_recv),
            (elders.at[col], elders, e_send, e_recv),
        )[k]
        return pltpu.make_async_remote_copy(
            src_ref=src, dst_ref=dst.at[slot],
            send_sem=send.at[d - 1], recv_sem=recv.at[slot],
            device_id=(row, lax.rem(col + d, n_coef)), device_id_type=MESH,
        )

    for k in range(2):
        for d in range(1, n_coef):
            gather_copy(k, d, col).start()

    def one_hot(line, count, value=1.0):
        wide = jnp.broadcast_to(line, (16, line.shape[1])).astype(BF)
        tall = jnp.concatenate([wide] * (count // 16), axis=0)
        iota = lax.broadcasted_iota(jnp.int32, tall.shape, 0).astype(jnp.float32).astype(BF)
        hit = jnp.full(tall.shape, value, jnp.float32).astype(BF)
        return jnp.where(tall == iota, hit, jnp.zeros_like(tall)).astype(HOT)

    half = 2 * pl.cdiv(noff, 4)

    def sign(j):
        return jnp.where(j < half, 1.0, -1.0)


    def fill_far(g):
        first = g * group
        target = target_ref[pl.ds(first, group), :]
        t = target - row * cd
        outer = (t < -cd) | (t >= 2 * cd)
        slot = jnp.where(t < 0, t + jnp.where(outer, 2 * cd, cd), t - jnp.where(outer, cd, 0))
        far = (target >= 0) & ((t < 0) | (t >= cd))
        slot = jnp.where(far, slot, -1).astype(jnp.float32)
        swap = ((t < -cd) | ((t >= cd) & (t < 2 * cd))).astype(jnp.float32)
        for j in range(group):
            hot_far[first + j] = one_hot(
                slot[j : j + 1], 2 * cd, sign(first + j)
            )
            outer_ref[first + j] = jnp.broadcast_to(
                swap[j : j + 1], (16, cd)
            ).astype(BF)

    def fill_near(g):
        first = g * group
        target = target_ref[pl.ds(first, group), :]
        t = target - row * cd
        slot = jnp.where((target >= 0) & (t >= 0) & (t < cd), t, -1).astype(jnp.float32)
        for j in range(group):
            hot_near[first + j] = one_hot(slot[j : j + 1], cd, sign(first + j))

    loads[2].wait()
    lax.fori_loop(0, noff // group, lambda g, _: fill_far(g), None)
    lax.fori_loop(0, noff // group, lambda g, _: fill_near(g), None)
    loads[3].wait()
    for t in range(tiles):
        leaf = (leaf_ref[t : t + 1, :] - row * cd).astype(jnp.float32)
        leaf_hot[:, t * lanes : (t + 1) * lanes] = one_hot(leaf, cd)

    for d in range(1, n_coef):
        gather_copy(0, d, lax.rem(col + d, n_coef)).wait_recv()
    loads[4].wait()

    poles = jnp.concatenate([gathered[j] for j in range(n_coef)], axis=0)
    def terms(first, last):
        high, low = halves(
            jnp.dot(ops_ref[first:last].reshape((last - first) * share, width), poles,
                    preferred_element_type=jnp.float32)
        )
        for j in range(first, last):
            here = slice((j - first) * share, (j - first + 1) * share)
            both = jnp.concatenate([high[here], low[here]], axis=0)
            keep = jnp.concatenate([outer_ref[j]] * (2 * share // 16), axis=0)
            rows_ref[j] = jnp.concatenate([both, both * keep], axis=0)

    cuts = (0, half, noff)
    for first, last in zip(cuts, cuts[1:]):
        terms(first, last)

    def window_copy(i, w):
        return pltpu.make_async_remote_copy(
            src_ref=out_buf.at[i], dst_ref=in_buf.at[i],
            send_sem=w_send.at[i], recv_sem=w_recv.at[i],
            device_id=(row + w, col), device_id_type=MESH,
        )

    def beside(ref, count, first, last):
        return jnp.concatenate([ref[j, :count] for j in range(first, last)], axis=1)

    def scatter(hot, count):
        plus, minus = (
            lax.dot_general(
                beside(rows_ref, count, *part), beside(hot, hot.shape[1], *part), NT,
                preferred_element_type=jnp.float32,
            )
            for part in ((0, half), (half, noff))
        )
        return plus - minus

    sums = scatter(hot_far, 4 * share)
    every = sums[:share] + sums[share : 2 * share]
    some = sums[2 * share : 3 * share] + sums[3 * share :]
    rest = every - some
    for i, part in enumerate((some[:, :cd], rest[:, cd:], rest[:, :cd], some[:, cd:])):
        out_buf[i] = part
    for i, w in enumerate(WINDOWS):
        @pl.when((row + w >= 0) & (row + w < n_cells))
        def _():
            window_copy(i, w).start()

    loads[5].wait()
    loads[6].wait()
    for d in range(1, n_coef):
        gather_copy(1, d, lax.rem(col + d, n_coef)).wait_recv()
    sums = scatter(hot_near, 2 * share)
    total = sums[:share] + sums[share:]

    held = (elders.shape[1], cd)
    child = lax.broadcasted_iota(jnp.int32, held, 1)
    family = child // 8 == lax.broadcasted_iota(jnp.int32, held, 0)
    family = family.astype(jnp.float32).astype(BF)
    wide_parents = jnp.concatenate(
        [
            lax.dot_general(elders[j], family, TN, preferred_element_type=jnp.float32)
            for j in range(n_coef)
        ],
        axis=0,
    )
    octant = lax.broadcasted_iota(jnp.int32, wide_parents.shape, 1) % 8
    spread = jnp.concatenate(
        [jnp.where(octant == j, wide_parents, 0.0).astype(BF) for j in range(8)], axis=0
    )
    shifts = jnp.concatenate([l2l_ref[j] for j in range(8)], axis=1)
    total = total + jnp.dot(shifts, spread, preferred_element_type=jnp.float32)
    local_ref[...] = total

    for i, w in enumerate(WINDOWS):
        @pl.when((row - w >= 0) & (row - w < n_cells))
        def _():
            window_copy(i, w).wait_recv()
            local_ref[...] += in_buf[i]

    columns = jnp.dot(
        jnp.concatenate(halves(local_ref[...]), axis=0), leaf_hot[...],
        preferred_element_type=jnp.float32,
    )
    columns = columns[:share] + columns[share:]
    partial = jnp.sum(columns * basis_ref[...].astype(jnp.float32), axis=0, keepdims=True)
    partials[col] = jnp.concatenate(
        [partial[:, t * lanes : (t + 1) * lanes] for t in range(tiles)], axis=0
    )

    def partial_copy(d, slot):
        return pltpu.make_async_remote_copy(
            src_ref=partials.at[slot], dst_ref=partials.at[slot],
            send_sem=p_send.at[d - 1], recv_sem=p_recv.at[slot],
            device_id=(row, lax.rem(col + d, n_coef)), device_id_type=MESH,
        )

    for d in range(1, n_coef):
        partial_copy(d, col).start()
    for d in range(1, n_coef):
        partial_copy(d, lax.rem(col + d, n_coef)).wait_recv()
    potential = partials[0]
    for j in range(1, n_coef):
        potential = potential + partials[j]
    pot_ref[...] = potential

    for d in range(1, n_coef):
        gather_copy(0, d, col).wait_send()
        gather_copy(1, d, col).wait_send()
        partial_copy(d, col).wait_send()
    for i, w in enumerate(WINDOWS):
        @pl.when((row + w >= 0) & (row + w < n_cells))
        def _():
            window_copy(i, w).wait_send()


def on_device(
    n_cells, n_coef,
    multipole, parent_local, m2l_ops, l2l_ops, target_cell, particle_leaf, particle_basis,
):
    share, cd = multipole.shape
    noff = m2l_ops.shape[0]
    particles = particle_leaf.shape[0]
    lanes = 128
    tiles = particles // lanes
    group = max(g for g in range(1, 33) if noff % g == 0)
    leaf = particle_leaf.reshape(tiles, lanes)
    nwin = len(WINDOWS)
    dma = pltpu.SemaphoreType.DMA
    vmem = pl.BlockSpec(memory_space=pltpu.VMEM)
    hbm = pl.BlockSpec(memory_space=pltpu.HBM)
    local, potential = pl.pallas_call(
        functools.partial(kernel, n_cells, n_coef, group),
        out_shape=(pltpu.VMEM((share, cd), jnp.float32), pltpu.VMEM((tiles, lanes), jnp.float32)),
        in_specs=[hbm] * 7,
        out_specs=(vmem, vmem),
        scratch_shapes=[
            pltpu.VMEM(m2l_ops.shape, m2l_ops.dtype),
            pltpu.VMEM(l2l_ops.shape, l2l_ops.dtype),
            pltpu.VMEM(target_cell.shape, target_cell.dtype),
            pltpu.VMEM(leaf.shape, leaf.dtype),
            pltpu.VMEM(particle_basis.shape, particle_basis.dtype),
            pltpu.VMEM((n_coef, share, cd), BF),
            pltpu.VMEM((n_coef,) + parent_local.shape[::-1], BF),
            pltpu.VMEM((noff, 2 * cd, cd), HOT),
            pltpu.VMEM((noff, cd, cd), HOT),
            pltpu.VMEM((cd, particles), HOT),
            pltpu.VMEM((noff, 16, cd), BF),
            pltpu.VMEM((noff, 4 * share, cd), BF),
            pltpu.VMEM((nwin, share, cd), jnp.float32),
            pltpu.VMEM((nwin, share, cd), jnp.float32),
            pltpu.VMEM((n_coef, tiles, lanes), jnp.float32),
            dma((7,)),
            dma((n_coef - 1,)),
            dma((n_coef,)),
            dma((n_coef - 1,)),
            dma((n_coef,)),
            dma((nwin,)),
            dma((nwin,)),
            dma((n_coef - 1,)),
            dma((n_coef,)),
        ],
        compiler_params=pltpu.CompilerParams(
            collective_id=0, has_side_effects=True, vmem_limit_bytes=60000000
        ),
    )(multipole, parent_local.T, m2l_ops, l2l_ops, target_cell, leaf, particle_basis)
    def put(a, b, c, d, sem):
        one = pltpu.make_async_copy(a, c, sem.at[0])
        two = pltpu.make_async_copy(b, d, sem.at[1])
        one.start()
        two.start()
        one.wait()
        two.wait()

    local = pltpu.with_memory_space_constraint(local, pltpu.VMEM)
    potential = pltpu.with_memory_space_constraint(potential, pltpu.VMEM)
    local, potential = pl.pallas_call(
        put,
        out_shape=(
            jax.ShapeDtypeStruct(local.shape, local.dtype),
            jax.ShapeDtypeStruct(potential.shape, potential.dtype),
        ),
        in_specs=[vmem, vmem],
        out_specs=(hbm, hbm),
        scratch_shapes=[dma((2,))],
    )(local, potential)
    return local, potential.reshape(particles)


def solution(mesh):
    return jax.shard_map(
        functools.partial(on_device, mesh.shape["cells"], mesh.shape["coef"]),
        mesh=mesh,
        in_specs=(
            P("coef", "cells"),
            P("coef", "cells"),
            P(None, "coef", None),
            P(None, "coef", None),
            P(None, "cells"),
            P("cells"),
            P("coef", "cells"),
        ),
        out_specs=(P("coef", "cells"), P("cells")),
        check_vma=False,
    )
```

```python
import functools

import jax
import jax.numpy as jnp
from jax import lax
from jax.experimental import pallas as pl
from jax.experimental.pallas import tpu as pltpu
from jax.sharding import PartitionSpec as P

WINDOWS = (-2, 2, -1, 1)
NT = (((1,), (1,)), ((), ()))
TN = (((0,), (0,)), ((), ()))
BF = jnp.bfloat16
HOT = jnp.float8_e4m3fn
MESH = pl.DeviceIdType.MESH


def halves(value):
    high = value.astype(BF)
    low = (value - high.astype(jnp.float32)).astype(BF)
    return high, low


def kernel(
    n_cells, n_coef, group,
    poles_hbm, parents_hbm, ops_hbm, l2l_hbm, target_hbm, leaf_hbm, basis_hbm,
    local_ref, pot_ref,
    ops_ref, l2l_ref, target_ref, leaf_ref, basis_ref,
    gathered, elders, hot_far, hot_near, leaf_hot, outer_ref, rows_ref,
    out_buf, in_buf, partials,
    load_sem, g_send, g_recv, e_send, e_recv, w_send, w_recv, p_send, p_recv,
):
    row = lax.axis_index("cells")
    col = lax.axis_index("coef")
    noff, share, width = ops_ref.shape
    cd = target_ref.shape[1]
    tiles, lanes = leaf_ref.shape

    barrier = pltpu.get_barrier_semaphore()
    for d in range(1, n_coef):
        pl.semaphore_signal(
            barrier, inc=1, device_id=(row, lax.rem(col + d, n_coef)), device_id_type=MESH
        )
    for w in WINDOWS:
        @pl.when((row + w >= 0) & (row + w < n_cells))
        def _():
            pl.semaphore_signal(barrier, inc=1, device_id=(row + w, col), device_id_type=MESH)
    loads = [
        pltpu.make_async_copy(src, dst, load_sem.at[i])
        for i, (src, dst) in enumerate(
            ((poles_hbm, gathered.at[col]), (parents_hbm, elders.at[col]),
             (target_hbm, target_ref), (leaf_hbm, leaf_ref), (ops_hbm, ops_ref),
             (l2l_hbm, l2l_ref), (basis_hbm, basis_ref))
        )
    ]
    for load in loads:
        load.start()

    peers = n_coef - 1
    for w in WINDOWS:
        peers = peers + ((row + w >= 0) & (row + w < n_cells)).astype(jnp.int32)
    pl.semaphore_wait(barrier, peers)
    loads[0].wait()
    loads[1].wait()

    def gather_copy(k, d, slot):
        src, dst, send, recv = (
            (gathered.at[col], gathered, g_send, g_recv),
            (elders.at[col], elders, e_send, e_recv),
        )[k]
        return pltpu.make_async_remote_copy(
            src_ref=src, dst_ref=dst.at[slot],
            send_sem=send.at[d - 1], recv_sem=recv.at[slot],
            device_id=(row, lax.rem(col + d, n_coef)), device_id_type=MESH,
        )

    for k in range(2):
        for d in range(1, n_coef):
            gather_copy(k, d, col).start()

    def one_hot(line, count, value=1.0):
        wide = jnp.broadcast_to(line, (16, line.shape[1])).astype(BF)
        tall = jnp.concatenate([wide] * (count // 16), axis=0)
        iota = lax.broadcasted_iota(jnp.int32, tall.shape, 0).astype(jnp.float32).astype(BF)
        hit = jnp.full(tall.shape, value, jnp.float32).astype(BF)
        return jnp.where(tall == iota, hit, jnp.zeros_like(tall)).astype(HOT)

    half = 2 * pl.cdiv(noff, 4)

    def sign(j):
        return jnp.where(j < half, 1.0, -1.0)


    def fill_far(g):
        first = g * group
        target = target_ref[pl.ds(first, group), :]
        t = target - row * cd
        outer = (t < -cd) | (t >= 2 * cd)
        slot = jnp.where(t < 0, t + jnp.where(outer, 2 * cd, cd), t - jnp.where(outer, cd, 0))
        far = (target >= 0) & ((t < 0) | (t >= cd))
        slot = jnp.where(far, slot, -1).astype(jnp.float32)
        swap = ((t < -cd) | ((t >= cd) & (t < 2 * cd))).astype(jnp.float32)
        for j in range(group):
            hot_far[first + j] = one_hot(
                slot[j : j + 1], 2 * cd, sign(first + j)
            )
            outer_ref[first + j] = jnp.broadcast_to(
                swap[j : j + 1], (16, cd)
            ).astype(BF)

    def fill_near(g):
        first = g * group
        target = target_ref[pl.ds(first, group), :]
        t = target - row * cd
        slot = jnp.where((target >= 0) & (t >= 0) & (t < cd), t, -1).astype(jnp.float32)
        for j in range(group):
            hot_near[first + j] = one_hot(slot[j : j + 1], cd, sign(first + j))

    loads[2].wait()
    lax.fori_loop(0, noff // group, lambda g, _: fill_far(g), None)
    lax.fori_loop(0, noff // group, lambda g, _: fill_near(g), None)
    loads[3].wait()
    for t in range(tiles):
        leaf = (leaf_ref[t : t + 1, :] - row * cd).astype(jnp.float32)
        leaf_hot[:, t * lanes : (t + 1) * lanes] = one_hot(leaf, cd)

    for d in range(1, n_coef):
        gather_copy(0, d, lax.rem(col + d, n_coef)).wait_recv()
    loads[4].wait()

    poles = jnp.concatenate([gathered[j] for j in range(n_coef)], axis=0)
    def terms(first, last):
        high, low = halves(
            jnp.dot(ops_ref[first:last].reshape((last - first) * share, width), poles,
                    preferred_element_type=jnp.float32)
        )
        for j in range(first, last):
            here = slice((j - first) * share, (j - first + 1) * share)
            both = jnp.concatenate([high[here], low[here]], axis=0)
            keep = jnp.concatenate([outer_ref[j]] * (2 * share // 16), axis=0)
            rows_ref[j] = jnp.concatenate([both, both * keep], axis=0)

    cuts = (0, half, noff)
    for first, last in zip(cuts, cuts[1:]):
        terms(first, last)

    def window_copy(i, w):
        return pltpu.make_async_remote_copy(
            src_ref=out_buf.at[i], dst_ref=in_buf.at[i],
            send_sem=w_send.at[i], recv_sem=w_recv.at[i],
            device_id=(row + w, col), device_id_type=MESH,
        )

    def beside(ref, count, first, last):
        return jnp.concatenate([ref[j, :count] for j in range(first, last)], axis=1)

    def scatter(hot, count):
        plus, minus = (
            lax.dot_general(
                beside(rows_ref, count, *part), beside(hot, hot.shape[1], *part), NT,
                preferred_element_type=jnp.float32,
            )
            for part in ((0, half), (half, noff))
        )
        return plus - minus

    sums = scatter(hot_far, 4 * share)
    every = sums[:share] + sums[share : 2 * share]
    some = sums[2 * share : 3 * share] + sums[3 * share :]
    rest = every - some
    for i, part in enumerate((some[:, :cd], rest[:, cd:], rest[:, :cd], some[:, cd:])):
        out_buf[i] = part
    for i, w in enumerate(WINDOWS):
        @pl.when((row + w >= 0) & (row + w < n_cells))
        def _():
            window_copy(i, w).start()

    loads[5].wait()
    loads[6].wait()
    for d in range(1, n_coef):
        gather_copy(1, d, lax.rem(col + d, n_coef)).wait_recv()
    sums = scatter(hot_near, 2 * share)
    total = sums[:share] + sums[share:]

    held = (elders.shape[1], cd)
    child = lax.broadcasted_iota(jnp.int32, held, 1)
    family = child // 8 == lax.broadcasted_iota(jnp.int32, held, 0)
    family = family.astype(jnp.float32).astype(BF)
    wide_parents = jnp.concatenate(
        [
            lax.dot_general(elders[j], family, TN, preferred_element_type=jnp.float32)
            for j in range(n_coef)
        ],
        axis=0,
    )
    octant = lax.broadcasted_iota(jnp.int32, wide_parents.shape, 1) % 8
    spread = jnp.concatenate(
        [jnp.where(octant == j, wide_parents, 0.0).astype(BF) for j in range(8)], axis=0
    )
    shifts = jnp.concatenate([l2l_ref[j] for j in range(8)], axis=1)
    total = total + jnp.dot(shifts, spread, preferred_element_type=jnp.float32)
    local_ref[...] = total

    for i, w in enumerate(WINDOWS):
        @pl.when((row - w >= 0) & (row - w < n_cells))
        def _():
            window_copy(i, w).wait_recv()
            local_ref[...] += in_buf[i]

    rows = jnp.concatenate(halves(local_ref[...]), axis=0)
    middle = pl.cdiv(tiles, 2)
    for first, last in ((0, middle), (middle, tiles)):
        reach = slice(first * lanes, last * lanes)
        columns = jnp.dot(rows, leaf_hot[:, reach], preferred_element_type=jnp.float32)
        columns = columns[:share] + columns[share:]
        partial = jnp.sum(
            columns * basis_ref[:, reach].astype(jnp.float32), axis=0, keepdims=True
        )
        partials[col, first:last] = jnp.concatenate(
            [partial[:, t * lanes : (t + 1) * lanes] for t in range(last - first)], axis=0
        )

    def partial_copy(d, slot):
        return pltpu.make_async_remote_copy(
            src_ref=partials.at[slot], dst_ref=partials.at[slot],
            send_sem=p_send.at[d - 1], recv_sem=p_recv.at[slot],
            device_id=(row, lax.rem(col + d, n_coef)), device_id_type=MESH,
        )

    for d in range(1, n_coef):
        partial_copy(d, col).start()
    for d in range(1, n_coef):
        partial_copy(d, lax.rem(col + d, n_coef)).wait_recv()
    potential = partials[0]
    for j in range(1, n_coef):
        potential = potential + partials[j]
    pot_ref[...] = potential

    for d in range(1, n_coef):
        gather_copy(0, d, col).wait_send()
        gather_copy(1, d, col).wait_send()
        partial_copy(d, col).wait_send()
    for i, w in enumerate(WINDOWS):
        @pl.when((row + w >= 0) & (row + w < n_cells))
        def _():
            window_copy(i, w).wait_send()


def on_device(
    n_cells, n_coef,
    multipole, parent_local, m2l_ops, l2l_ops, target_cell, particle_leaf, particle_basis,
):
    share, cd = multipole.shape
    noff = m2l_ops.shape[0]
    particles = particle_leaf.shape[0]
    lanes = 128
    tiles = particles // lanes
    group = max(g for g in range(1, 33) if noff % g == 0)
    leaf = particle_leaf.reshape(tiles, lanes)
    nwin = len(WINDOWS)
    dma = pltpu.SemaphoreType.DMA
    vmem = pl.BlockSpec(memory_space=pltpu.VMEM)
    hbm = pl.BlockSpec(memory_space=pltpu.HBM)
    local, potential = pl.pallas_call(
        functools.partial(kernel, n_cells, n_coef, group),
        out_shape=(pltpu.VMEM((share, cd), jnp.float32), pltpu.VMEM((tiles, lanes), jnp.float32)),
        in_specs=[hbm] * 7,
        out_specs=(vmem, vmem),
        scratch_shapes=[
            pltpu.VMEM(m2l_ops.shape, m2l_ops.dtype),
            pltpu.VMEM(l2l_ops.shape, l2l_ops.dtype),
            pltpu.VMEM(target_cell.shape, target_cell.dtype),
            pltpu.VMEM(leaf.shape, leaf.dtype),
            pltpu.VMEM(particle_basis.shape, particle_basis.dtype),
            pltpu.VMEM((n_coef, share, cd), BF),
            pltpu.VMEM((n_coef,) + parent_local.shape[::-1], BF),
            pltpu.VMEM((noff, 2 * cd, cd), HOT),
            pltpu.VMEM((noff, cd, cd), HOT),
            pltpu.VMEM((cd, particles), HOT),
            pltpu.VMEM((noff, 16, cd), BF),
            pltpu.VMEM((noff, 4 * share, cd), BF),
            pltpu.VMEM((nwin, share, cd), jnp.float32),
            pltpu.VMEM((nwin, share, cd), jnp.float32),
            pltpu.VMEM((n_coef, tiles, lanes), jnp.float32),
            dma((7,)),
            dma((n_coef - 1,)),
            dma((n_coef,)),
            dma((n_coef - 1,)),
            dma((n_coef,)),
            dma((nwin,)),
            dma((nwin,)),
            dma((n_coef - 1,)),
            dma((n_coef,)),
        ],
        compiler_params=pltpu.CompilerParams(
            collective_id=0, has_side_effects=True, vmem_limit_bytes=60000000
        ),
    )(multipole, parent_local.T, m2l_ops, l2l_ops, target_cell, leaf, particle_basis)
    def put(a, b, c, d, sem):
        one = pltpu.make_async_copy(a, c, sem.at[0])
        two = pltpu.make_async_copy(b, d, sem.at[1])
        one.start()
        two.start()
        one.wait()
        two.wait()

    local = pltpu.with_memory_space_constraint(local, pltpu.VMEM)
    potential = pltpu.with_memory_space_constraint(potential, pltpu.VMEM)
    local, potential = pl.pallas_call(
        put,
        out_shape=(
            jax.ShapeDtypeStruct(local.shape, local.dtype),
            jax.ShapeDtypeStruct(potential.shape, potential.dtype),
        ),
        in_specs=[vmem, vmem],
        out_specs=(hbm, hbm),
        scratch_shapes=[dma((2,))],
    )(local, potential)
    return local, potential.reshape(particles)


def solution(mesh):
    return jax.shard_map(
        functools.partial(on_device, mesh.shape["cells"], mesh.shape["coef"]),
        mesh=mesh,
        in_specs=(
            P("coef", "cells"),
            P("coef", "cells"),
            P(None, "coef", None),
            P(None, "coef", None),
            P(None, "cells"),
            P("cells"),
            P("coef", "cells"),
        ),
        out_specs=(P("coef", "cells"), P("cells")),
        check_vma=False,
    )
```
